32 devices in a mesh: seq: 8 (over z, y), head: 4 (over x, core).
Axes of the slice: x: 2, y: 2, z: 4, core: 2. Of those that a mesh axis runs over, the one named last changes fastest.
Arguments:
- doc_lengths: int32 [32], P(('seq', 'head')), may hold values from 1 to 2688, 6144 in all
- queries: bfloat16 [6144, 8192], P('seq', 'head'), may hold values from -24 to 24
- key_states: bfloat16 [6144, 1024], P('seq', 'head'), may hold values from -24 to 24
- value_states: bfloat16 [6144, 1024], P('seq', 'head'), may hold values from -6 to 6
Outputs:
- attended: bfloat16 [6144, 8192], P('seq', 'head')
The draws below stay inside these ranges and needn't reach their ends.
Inputs may be any that keep to these rules, and one draw needn't show every extreme that they name: `doc_lengths`: the 32 lengths sum to 6144; the largest is exactly 2688.
All inputs are finite; a program needn't handle non-finite values. No bound on the sum of `doc_lengths` on one device may be relied on, other than what follows from the above.
Results may differ from the reference program's by a relative error of at most 0.0028.
Values may be sent and summed in bfloat16 or wider, within the bound.
A program may use at most 64 MiB of HBM per device.

```python
import math
import jax
import jax.numpy as jnp
import numpy as np
from jax import lax

HD = 128
QH = 64
KVH = 8
TILE = 128
GROUP = 8
TOKENS = 6144
DOCS = 32
LONGEST = 2688


def draw_queries(key, part):
    drawn = jnp.clip(jax.random.normal(jax.random.fold_in(key, 1), (TOKENS, QH * HD)), -6.0, 6.0)
    return drawn.astype(jnp.bfloat16)


def draw_key_states(key, part):
    drawn = jnp.clip(jax.random.normal(jax.random.fold_in(key, 2), (TOKENS, KVH * HD)), -6.0, 6.0)
    return drawn.astype(jnp.bfloat16)


def shard_levels(rng, shape, cuts, smallest, top_value):
    def one(dim, shards_of):
        steps = jax.random.uniform(jax.random.fold_in(jax.random.fold_in(rng, 6), dim), (shards_of,), jnp.float32, smallest / len(cuts), top_value / len(cuts))
        return jnp.repeat(jnp.exp(steps), shape[dim] // shards_of).reshape((-1,) + (1,) * (len(shape) - dim - 1))

    gain = one(*cuts[0])
    for cut in cuts[1:]:
        gain = gain * one(*cut)
    return gain


def length_profile(number_of, total, bound, skew):
    weights = [(1 << 20) // math.isqrt(grade ** skew) + 1 for grade in range(2, number_of + 1)]
    rest, counts = total - bound - (number_of - 1), [1] * (number_of - 1)
    while rest > 0:
        candidates = [i for i in range(number_of - 1) if counts[i] < bound]
        whole, remaining = sum([weights[i] for i in candidates]), rest
        for i in candidates:
            extra = min(bound - counts[i], max(1, remaining * weights[i] // whole), rest)
            counts[i] = counts[i] + extra
            rest = rest - extra
    return np.array([bound] + counts)


def ragged(rng, number_of, total, most, skew):
    if number_of == 2:
        one = jax.random.randint(rng, (), max(1, total - most), min(most, total - 1) + 1)
        return jnp.stack([one, total - one])
    tallies = jnp.asarray(length_profile(number_of, total, most, skew), jnp.int32)
    pairs = (number_of - 1) // 2
    giver, taker = tallies[1:1 + 2 * pairs:2], tallies[2:2 + 2 * pairs:2]
    slack = jnp.minimum(giver - 1, most - taker)
    shifted = jax.random.randint(jax.random.fold_in(rng, 1), (pairs,), 0, 1 << 20) % (slack + 1)
    tallies = tallies.at[1:1 + 2 * pairs:2].set(giver - shifted).at[2:2 + 2 * pairs:2].set(taker + shifted)
    return tallies[jax.random.permutation(jax.random.fold_in(rng, 2), number_of)]


def centred(stream_key, shape, deviation, reach, pieces=(), kind=jnp.bfloat16):
    level = shard_levels(stream_key, shape, pieces, -0.22, 0.18) if pieces else 1.0
    values = jax.random.normal(stream_key, shape, jnp.float32) * deviation * level
    return jnp.minimum(jnp.maximum(values, -reach), reach).astype(kind)


def setup_inputs(seed: int = 0) -> dict:
    splits = jax.random.split(jax.random.key(seed), 5)
    return {
        "doc_lengths": ragged(splits[0], DOCS, TOKENS, LONGEST, 2).astype(jnp.int32),
        "queries": draw_queries(jax.random.fold_in(splits[4], 71), 0),
        "key_states": draw_key_states(jax.random.fold_in(splits[4], 71), 0),
        "value_states": centred(splits[3], (TOKENS, KVH * HD), 1.0, 6.0, ((0, 8), (1, 4))),
    }


far_below = -1e+30

def document_start(positions, doc_ends, doc_lengths):
    finished = doc_ends[None, :] <= positions[:, None]
    return lax.optimization_barrier(jnp.sum(jnp.where(finished, doc_lengths[None, :], 0), axis=1)).astype(jnp.int32)

def reference(doc_lengths, queries, key_states, value_states):
    doc_ends = jnp.cumsum(doc_lengths).astype(jnp.int32)
    key_span = LONGEST + TILE
    front_zeros = jnp.zeros((LONGEST, KVH * HD), key_states.dtype)
    padded_keys = jnp.concatenate([front_zeros, key_states], axis=0)
    padded_values = jnp.concatenate([front_zeros, value_states], axis=0)
    score_scale = 1.0 / math.sqrt(HD)

    def one_tile(tile_index):
        first_row = (tile_index * TILE).astype(jnp.int32)
        query_tile = lax.dynamic_slice_in_dim(queries, first_row, TILE, 0).reshape(TILE, KVH, GROUP, HD).astype(jnp.float32)
        key_window = lax.dynamic_slice_in_dim(padded_keys, first_row, key_span, 0).reshape(key_span, KVH, HD).astype(jnp.float32)
        value_window = lax.dynamic_slice_in_dim(padded_values, first_row, key_span, 0).reshape(key_span, KVH, HD).astype(jnp.float32)
        query_pos = first_row + jnp.arange(TILE, dtype=jnp.int32)
        key_pos = first_row - LONGEST + jnp.arange(key_span, dtype=jnp.int32)
        starts = document_start(query_pos, doc_ends, doc_lengths)
        visible = (key_pos[None, :] >= starts[:, None]) & (key_pos[None, :] <= query_pos[:, None])
        scores = jnp.einsum('qhgd,khd->hgqk', query_tile, key_window) * score_scale
        scores = jnp.where(visible, scores, far_below)
        row_max = lax.optimization_barrier(jnp.max(scores, axis=-1, keepdims=True))
        weights = jnp.where(visible, jnp.exp(scores - row_max), 0.0)
        weight_sum = lax.optimization_barrier(jnp.sum(weights, axis=-1, keepdims=True))
        rounded = lax.optimization_barrier(weights.astype(jnp.bfloat16))
        mixed_out = jnp.einsum('hgqk,khd->hgqd', rounded.astype(jnp.float32), value_window) / weight_sum
        return mixed_out.transpose(2, 0, 1, 3).reshape(TILE, QH * HD).astype(jnp.bfloat16)
    all_tiles = lax.map(one_tile, jnp.arange(TOKENS // TILE, dtype=jnp.int32))
    return all_tiles.reshape(TOKENS, QH * HD)
```

```python
import functools
import math

import jax
import jax.numpy as jnp
from jax import lax
from jax.experimental import pallas as pl
from jax.experimental.pallas import tpu as pltpu
from jax.sharding import PartitionSpec as P

HD = 128
TILE = 128
KB = 256
CHUNK = 256
LONGEST = 2688
PAD = 128
FAR_BELOW = -1e30


def document_start(positions, doc_ends, doc_lengths):
    finished = doc_ends[None, :] <= positions[:, None]
    return jnp.sum(jnp.where(finished, doc_lengths[None, :], 0), axis=1)


def attend(
    n_pieces,
    piece_rows,
    local_row,
    group,
    plain_ref,
    total_ref,
    starts_ref,
    q_ref,
    *rest,
):
    pieces = rest[:n_pieces]
    out_ref = rest[n_pieces]
    win, qs, acc, m_ref, l_ref, sems = rest[n_pieces + 1 :]
    head = pl.program_id(0)
    tile = pl.program_id(1)
    heads = pl.num_programs(0)
    width = group * TILE
    n_chunks = width // CHUNK
    kv_heads = win.shape[1]

    @pl.when((head == 0) & (tile == 0))
    def _():
        copies = []
        row = PAD
        for i in range(n_pieces):
            for kv in range(2):
                for c in range(kv_heads):
                    copy = pltpu.make_async_copy(
                        pieces[i].at[kv, :, pl.ds(c * HD, HD)],
                        win.at[kv, c, pl.ds(row, piece_rows[i]), :],
                        sems.at[i, kv, c],
                    )
                    copy.start()
                    copies.append(copy)
            row += piece_rows[i]
        for kv in range(2):
            for c in range(kv_heads):
                win[kv, c, 0:PAD, :] = jnp.zeros((PAD, HD), win.dtype)
        for copy in copies:
            copy.wait()

    for g in range(group):
        qs[g * TILE : (g + 1) * TILE, :] = q_ref[:, g * HD : (g + 1) * HD]

    scale = 1.0 / math.sqrt(HD)
    first_row = pl.multiple_of(PAD + local_row + tile * TILE, TILE)
    starts = starts_ref[pl.ds(tile, 1), :]

    def block(begin, rows, masked, causal):
        keys = win[0, head, pl.ds(begin, rows), :]
        values_t = win[1, head, pl.ds(begin, rows), :].T
        for i in range(n_chunks):
            lanes = slice(i * CHUNK, (i + 1) * CHUNK)
            scores = lax.dot_general(
                keys, qs[lanes, :], (((1,), (1,)), ((), ())), preferred_element_type=jnp.float32
            )
            if masked:
                key_row = begin + lax.broadcasted_iota(jnp.int32, (rows, CHUNK), 0)
                visible = key_row >= starts
                if causal:
                    query_row = first_row + lax.broadcasted_iota(
                        jnp.int32, (rows, CHUNK), 1
                    ) % TILE
                    visible = visible & (key_row <= query_row)
                scores = jnp.where(visible, scores, FAR_BELOW)
            top = jnp.max(scores, axis=0, keepdims=True)
            if causal:
                new_max = top
            else:
                old_max = m_ref[:, lanes]
                new_max = jnp.maximum(old_max, top)
            weights = jnp.exp((scores - new_max) * scale)
            part_sum = jnp.sum(weights, axis=0, keepdims=True)
            update = jnp.dot(
                values_t, weights.astype(jnp.bfloat16), preferred_element_type=jnp.float32
            )
            if causal:
                l_ref[:, lanes] = part_sum
                acc[:, lanes] = update
            else:
                shrink = jnp.exp((old_max - new_max) * scale)
                l_ref[:, lanes] = l_ref[:, lanes] * shrink + part_sum
                acc[:, lanes] = acc[:, lanes] * shrink + update
            m_ref[:, lanes] = new_max

    block(first_row, TILE, True, True)

    def back(masked, j, carry):
        begin = pl.multiple_of(first_row - (j + 1) * KB, TILE)
        block(begin, KB, masked, False)
        return carry

    plain = plain_ref[tile]
    lax.fori_loop(0, plain, functools.partial(back, False), 0)
    lax.fori_loop(plain, total_ref[tile], functools.partial(back, True), 0)

    for g in range(group):
        lanes = slice(g * TILE, (g + 1) * TILE)
        result = acc[:, lanes] / l_ref[:, lanes]
        out_ref[:, g * HD : (g + 1) * HD] = result.T.astype(jnp.bfloat16)


def gather_window(stacked, count):
    rows = stacked.shape[1]
    reach = LONGEST - 3 * rows

    def hop(value, pairs):
        return lax.ppermute(value, "seq", pairs)

    ahead = [(r, r + 2) for r in range(count - 2)]
    odd_ahead = [(r, r + 2) for r in range(1, count - 2, 2)]
    up = [(r, r + 1) for r in range(0, count, 2)]
    down = [(r + 1, r) for r in range(0, count, 2)]
    rank = lax.axis_index("seq")
    is_even = rank % 2 == 0
    two = hop(stacked, ahead)
    pair = hop(stacked, up)
    swapped = hop(two, up + down)
    far_hi = hop(two[:, rows - reach :], ahead)
    far_lo = hop(two[:, : rows - reach], odd_ahead)
    cross_hi = hop(far_hi, down)
    cross_lo = hop(far_lo, down)
    one = jnp.where(is_even, swapped, pair)
    three_hi = jnp.where(is_even, cross_hi, swapped[:, rows - reach :])
    three_lo = jnp.where(is_even, cross_lo, swapped[:, : rows - reach])
    return [far_hi, three_lo, three_hi, two, one, stacked]


def body(doc_lengths, queries, key_states, value_states):
    seq_rank = lax.axis_index("seq")
    rows = queries.shape[0]
    tiles = rows // TILE
    kv_heads = key_states.shape[1] // HD
    group = queries.shape[1] // (kv_heads * HD)
    width = group * TILE
    every_length = lax.all_gather(doc_lengths, ("seq", "head"), axis=0, tiled=True)
    doc_ends = jnp.cumsum(every_length)
    positions = seq_rank * rows + jnp.arange(rows, dtype=jnp.int32)
    starts = document_start(positions, doc_ends, every_length)
    pieces = gather_window(jnp.stack([key_states, value_states], axis=0), lax.axis_size("seq"))
    piece_rows = [piece.shape[1] for piece in pieces]
    local_row = sum(piece_rows[:-1])
    start_rows = (starts - seq_rank * rows + local_row + PAD).reshape(tiles, TILE)
    tile_rows = PAD + local_row + jnp.arange(tiles, dtype=jnp.int32) * TILE
    total = jnp.maximum(0, tile_rows - start_rows[:, 0] + KB - 1) // KB
    plain = jnp.maximum(0, tile_rows - start_rows[:, -1]) // KB
    starts_wide = jnp.tile(start_rows, (1, CHUNK // TILE))

    win_rows = PAD + sum(piece_rows)
    kernel = functools.partial(attend, len(pieces), piece_rows, local_row, group)
    return pl.pallas_call(
        kernel,
        out_shape=jax.ShapeDtypeStruct(queries.shape, jnp.bfloat16),
        grid_spec=pltpu.PrefetchScalarGridSpec(
            num_scalar_prefetch=2,
            grid=(kv_heads, tiles),
            in_specs=[
                pl.BlockSpec((tiles, CHUNK), lambda c, t, *_: (0, 0)),
                pl.BlockSpec((TILE, width), lambda c, t, *_: (t, c)),
            ]
            + [pl.BlockSpec(memory_space=pl.ANY)] * len(pieces),
            out_specs=pl.BlockSpec((TILE, width), lambda c, t, *_: (t, c)),
            scratch_shapes=[
                pltpu.VMEM((2, kv_heads, win_rows, HD), jnp.bfloat16),
                pltpu.VMEM((width, HD), jnp.bfloat16),
                pltpu.VMEM((HD, width), jnp.float32),
                pltpu.VMEM((1, width), jnp.float32),
                pltpu.VMEM((1, width), jnp.float32),
                pltpu.SemaphoreType.DMA((len(pieces), 2, kv_heads)),
            ],
        ),
        compiler_params=pltpu.CompilerParams(
            dimension_semantics=("arbitrary", "arbitrary"), vmem_limit_bytes=48 * 1024 * 1024
        ),
    )(plain, total, starts_wide, queries, *pieces)


def solution(mesh):
    return jax.shard_map(
        body,
        mesh=mesh,
        in_specs=(P(("seq", "head")), P("seq", "head"), P("seq", "head"), P("seq", "head")),
        out_specs=P("seq", "head"),
        check_vma=False,
    )
```

```python
import functools
import math

import jax
import jax.numpy as jnp
from jax import lax
from jax.experimental import pallas as pl
from jax.experimental.pallas import tpu as pltpu
from jax.sharding import PartitionSpec as P

HD = 128
TILE = 128
KB = 512
CHUNK = 256
AHEAD = 4
LONGEST = 2688
PAD = 384
FAR_BELOW = -1e30


def document_start(positions, doc_ends, doc_lengths):
    finished = doc_ends[None, :] <= positions[:, None]
    return jnp.sum(jnp.where(finished, doc_lengths[None, :], 0), axis=1)


def attend(
    n_pieces,
    piece_rows,
    local_row,
    group,
    plain_ref,
    total_ref,
    starts_ref,
    q_ref,
    *rest,
):
    pieces = rest[:n_pieces]
    out_ref = rest[n_pieces]
    win, qs, acc, m_ref, l_ref, sems = rest[n_pieces + 1 :]
    head = pl.program_id(0)
    tile = pl.program_id(1)
    heads = pl.num_programs(0)
    width = group * TILE
    n_chunks = width // CHUNK
    kv_heads = win.shape[1]

    @pl.when((head == 0) & (tile == 0))
    def _():
        copies = []
        row = PAD
        for i in range(n_pieces):
            for kv in range(2):
                for c in range(kv_heads):
                    copy = pltpu.make_async_copy(
                        pieces[i].at[kv, :, pl.ds(c * HD, HD)],
                        win.at[kv, c, pl.ds(row, piece_rows[i]), :],
                        sems.at[i, kv, c],
                    )
                    copy.start()
                    copies.append(copy)
            row += piece_rows[i]
        for kv in range(2):
            for c in range(kv_heads):
                win[kv, c, 0:PAD, :] = jnp.zeros((PAD, HD), win.dtype)
        for copy in copies:
            copy.wait()

    for g in range(group):
        qs[g * TILE : (g + 1) * TILE, :] = q_ref[:, g * HD : (g + 1) * HD]

    scale = math.log2(math.e) / math.sqrt(HD)
    first_row = pl.multiple_of(PAD + local_row + tile * TILE, TILE)
    starts = starts_ref[pl.ds(tile, 1), :]

    def block(begin, rows, masked, causal):
        keys = win[0, head, pl.ds(begin, rows), :]
        values_t = win[1, head, pl.ds(begin, rows), :].T
        def score(i):
            lanes = slice(i * CHUNK, (i + 1) * CHUNK)
            return lax.dot_general(
                keys, qs[lanes, :], (((1,), (1,)), ((), ())), preferred_element_type=jnp.float32
            )

        ready = [score(i) for i in range(min(AHEAD, n_chunks))]
        for i in range(n_chunks):
            lanes = slice(i * CHUNK, (i + 1) * CHUNK)
            if i + AHEAD < n_chunks:
                ready.append(score(i + AHEAD))
            scores = ready.pop(0)
            if masked:
                key_row = begin + lax.broadcasted_iota(jnp.int32, (rows, CHUNK), 0)
                visible = key_row >= starts
                if causal:
                    query_row = first_row + lax.broadcasted_iota(
                        jnp.int32, (rows, CHUNK), 1
                    ) % TILE
                    visible = visible & (key_row <= query_row)
                scores = jnp.where(visible, scores, FAR_BELOW)
            top = jnp.max(scores, axis=0, keepdims=True)
            if causal:
                new_max = top
            else:
                old_max = m_ref[:, lanes]
                new_max = jnp.maximum(old_max, top)
            weights = jnp.exp2((scores - new_max) * scale)
            part_sum = jnp.sum(weights, axis=0, keepdims=True)
            update = jnp.dot(
                values_t, weights.astype(jnp.bfloat16), preferred_element_type=jnp.float32
            )
            if causal:
                l_ref[:, lanes] = part_sum
                acc[:, lanes] = update
            else:
                shrink = jnp.exp2((old_max - new_max) * scale)
                l_ref[:, lanes] = l_ref[:, lanes] * shrink + part_sum
                acc[:, lanes] = acc[:, lanes] * shrink + update
            m_ref[:, lanes] = new_max

    block(first_row, TILE, True, True)

    def back(masked, j, carry):
        begin = pl.multiple_of(first_row - (j + 1) * KB, TILE)
        block(begin, KB, masked, False)
        return carry

    plain = plain_ref[tile]
    lax.fori_loop(0, plain, functools.partial(back, False), 0)
    lax.fori_loop(plain, total_ref[tile], functools.partial(back, True), 0)

    for g in range(group):
        lanes = slice(g * TILE, (g + 1) * TILE)
        result = acc[:, lanes] / l_ref[:, lanes]
        out_ref[:, g * HD : (g + 1) * HD] = result.T.astype(jnp.bfloat16)


def gather_window(stacked, count):
    rows = stacked.shape[1]
    reach = LONGEST - 3 * rows

    def hop(value, pairs):
        return lax.ppermute(value, "seq", pairs)

    ahead = [(r, r + 2) for r in range(count - 2)]
    odd_ahead = [(r, r + 2) for r in range(1, count - 2, 2)]
    up = [(r, r + 1) for r in range(0, count, 2)]
    down = [(r + 1, r) for r in range(0, count, 2)]
    rank = lax.axis_index("seq")
    is_even = rank % 2 == 0
    two = hop(stacked, ahead)
    pair = hop(stacked, up)
    swapped = hop(two, up + down)
    far_hi = hop(two[:, rows - reach :], ahead)
    far_lo = hop(two[:, : rows - reach], odd_ahead)
    cross_hi = hop(far_hi, down)
    cross_lo = hop(far_lo, down)
    one = jnp.where(is_even, swapped, pair)
    three_hi = jnp.where(is_even, cross_hi, swapped[:, rows - reach :])
    three_lo = jnp.where(is_even, cross_lo, swapped[:, : rows - reach])
    return [far_hi, three_lo, three_hi, two, one, stacked]


def body(doc_lengths, queries, key_states, value_states):
    seq_rank = lax.axis_index("seq")
    rows = queries.shape[0]
    tiles = rows // TILE
    kv_heads = key_states.shape[1] // HD
    group = queries.shape[1] // (kv_heads * HD)
    width = group * TILE
    every_length = lax.all_gather(doc_lengths, ("seq", "head"), axis=0, tiled=True)
    positions = seq_rank * rows + jnp.arange(rows, dtype=jnp.int32)
    stacked = jnp.stack([key_states, value_states], axis=0)
    every_length, stacked = lax.optimization_barrier((every_length, stacked))
    doc_ends = jnp.cumsum(every_length)
    pieces = gather_window(stacked, lax.axis_size("seq"))
    starts = document_start(positions, doc_ends, every_length)
    piece_rows = [piece.shape[1] for piece in pieces]
    local_row = sum(piece_rows[:-1])
    start_rows = (starts - seq_rank * rows + local_row + PAD).reshape(tiles, TILE)
    tile_rows = PAD + local_row + jnp.arange(tiles, dtype=jnp.int32) * TILE
    total = jnp.maximum(0, tile_rows - start_rows[:, 0] + KB - 1) // KB
    plain = jnp.maximum(0, tile_rows - start_rows[:, -1]) // KB
    starts_wide = jnp.tile(start_rows, (1, CHUNK // TILE))

    win_rows = PAD + sum(piece_rows)
    kernel = functools.partial(attend, len(pieces), piece_rows, local_row, group)
    return pl.pallas_call(
        kernel,
        out_shape=jax.ShapeDtypeStruct(queries.shape, jnp.bfloat16),
        grid_spec=pltpu.PrefetchScalarGridSpec(
            num_scalar_prefetch=2,
            grid=(kv_heads, tiles),
            in_specs=[
                pl.BlockSpec((tiles, CHUNK), lambda c, t, *_: (0, 0)),
                pl.BlockSpec((TILE, width), lambda c, t, *_: (t, c)),
            ]
            + [pl.BlockSpec(memory_space=pl.ANY)] * len(pieces),
            out_specs=pl.BlockSpec((TILE, width), lambda c, t, *_: (t, c)),
            scratch_shapes=[
                pltpu.VMEM((2, kv_heads, win_rows, HD), jnp.bfloat16),
                pltpu.VMEM((width, HD), jnp.bfloat16),
                pltpu.VMEM((HD, width), jnp.float32),
                pltpu.VMEM((1, width), jnp.float32),
                pltpu.VMEM((1, width), jnp.float32),
                pltpu.SemaphoreType.DMA((len(pieces), 2, kv_heads)),
            ],
        ),
        compiler_params=pltpu.CompilerParams(
            dimension_semantics=("arbitrary", "arbitrary"), vmem_limit_bytes=48 * 1024 * 1024
        ),
    )(plain, total, starts_wide, queries, *pieces)


def solution(mesh):
    return jax.shard_map(
        body,
        mesh=mesh,
        in_specs=(P(("seq", "head")), P("seq", "head"), P("seq", "head"), P("seq", "head")),
        out_specs=P("seq", "head"),
        check_vma=False,
    )
```

```python
import functools
import math

import jax
import jax.numpy as jnp
from jax import lax
from jax.experimental import pallas as pl
from jax.experimental.pallas import tpu as pltpu
from jax.sharding import PartitionSpec as P

HD = 128
TILE = 128
KB = 512
CHUNK = 256
AHEAD = 4
LONGEST = 2688
PAD = 384
FAR_BELOW = -1e30


def document_start(positions, doc_ends, doc_lengths):
    finished = doc_ends[None, :] <= positions[:, None]
    return jnp.sum(jnp.where(finished, doc_lengths[None, :], 0), axis=1)


def attend(
    n_pieces,
    piece_rows,
    local_row,
    group,
    plain_ref,
    total_ref,
    starts_ref,
    q_ref,
    *rest,
):
    pieces = rest[:n_pieces]
    out_ref = rest[n_pieces]
    win, qs, acc, m_ref, l_ref, sems = rest[n_pieces + 1 :]
    head = pl.program_id(0)
    tile = pl.program_id(1)
    heads = pl.num_programs(0)
    width = group * TILE
    n_chunks = width // CHUNK
    kv_heads = win.shape[1]

    @pl.when((head == 0) & (tile == 0))
    def _():
        copies = []
        row = PAD
        for i in range(n_pieces):
            for kv in range(2):
                for c in range(kv_heads):
                    copy = pltpu.make_async_copy(
                        pieces[i].at[kv, :, pl.ds(c * HD, HD)],
                        win.at[kv, c, pl.ds(row, piece_rows[i]), :],
                        sems.at[i, kv, c],
                    )
                    copy.start()
                    copies.append(copy)
            row += piece_rows[i]
        for kv in range(2):
            for c in range(kv_heads):
                win[kv, c, 0:PAD, :] = jnp.zeros((PAD, HD), win.dtype)
        for copy in copies:
            copy.wait()

    for g in range(group):
        qs[g * TILE : (g + 1) * TILE, :] = q_ref[:, g * HD : (g + 1) * HD]

    scale = math.log2(math.e) / math.sqrt(HD)
    first_row = pl.multiple_of(PAD + local_row + tile * TILE, TILE)
    starts = starts_ref[pl.ds(tile, 1), :]

    def block(begin, rows, masked, causal):
        keys = win[0, head, pl.ds(begin, rows), :]
        values_t = win[1, head, pl.ds(begin, rows), :].T
        def score(i):
            lanes = slice(i * CHUNK, (i + 1) * CHUNK)
            return lax.dot_general(
                keys, qs[lanes, :], (((1,), (1,)), ((), ())), preferred_element_type=jnp.float32
            )

        ready = [score(i) for i in range(min(AHEAD, n_chunks))]
        for i in range(n_chunks):
            lanes = slice(i * CHUNK, (i + 1) * CHUNK)
            if i + AHEAD < n_chunks:
                ready.append(score(i + AHEAD))
            scores = ready.pop(0)
            if masked:
                key_row = begin + lax.broadcasted_iota(jnp.int32, (rows, CHUNK), 0)
                visible = key_row >= starts
                if causal:
                    query_row = first_row + lax.broadcasted_iota(
                        jnp.int32, (rows, CHUNK), 1
                    ) % TILE
                    visible = visible & (key_row <= query_row)
                scores = jnp.where(visible, scores, FAR_BELOW)
            top = jnp.max(scores, axis=0, keepdims=True)
            if causal:
                new_max = top
            else:
                old_max = m_ref[:, lanes]
                new_max = jnp.maximum(old_max, top)
            weights = jnp.exp2((scores - new_max) * scale)
            part_sum = jnp.sum(weights, axis=0, keepdims=True)
            update = jnp.dot(
                values_t, weights.astype(jnp.bfloat16), preferred_element_type=jnp.float32
            )
            if causal:
                l_ref[:, lanes] = part_sum
                acc[:, lanes] = update
            else:
                shrink = jnp.exp2((old_max - new_max) * scale)
                l_ref[:, lanes] = l_ref[:, lanes] * shrink + part_sum
                acc[:, lanes] = acc[:, lanes] * shrink + update
            m_ref[:, lanes] = new_max

    block(first_row, TILE, True, True)

    def back(masked, j, carry):
        begin = pl.multiple_of(first_row - (j + 1) * KB, TILE)
        block(begin, KB, masked, False)
        return carry

    plain = plain_ref[tile]
    lax.fori_loop(0, plain, functools.partial(back, False), 0)
    lax.fori_loop(plain, total_ref[tile], functools.partial(back, True), 0)

    for g in range(group):
        lanes = slice(g * TILE, (g + 1) * TILE)
        result = acc[:, lanes] / l_ref[:, lanes]
        out_ref[:, g * HD : (g + 1) * HD] = result.T.astype(jnp.bfloat16)


def doubling_gather(part, axis):
    count = lax.axis_size(axis)
    each = part.shape[0]
    held, have = part, 1
    while have < count:
        more = min(have, count - have)
        pairs = [((r + have) % count, r) for r in range(count)]
        held = jnp.concatenate([held, lax.ppermute(held[: more * each], axis, pairs)])
        have += more
    first = (count - lax.axis_index(axis)) * each
    return lax.dynamic_slice_in_dim(jnp.concatenate([held, held]), first, count * each, 0)


def gather_window(stacked, count):
    rows = stacked.shape[1]
    reach = LONGEST - 3 * rows

    def hop(value, pairs):
        return lax.ppermute(value, "seq", pairs)

    ahead = [(r, r + 2) for r in range(count - 2)]
    odd_ahead = [(r, r + 2) for r in range(1, count - 2, 2)]
    up = [(r, r + 1) for r in range(0, count, 2)]
    down = [(r + 1, r) for r in range(0, count, 2)]
    rank = lax.axis_index("seq")
    is_even = rank % 2 == 0
    two = hop(stacked, ahead)
    pair = hop(stacked, up)
    swapped = hop(two, up + down)
    far_hi = hop(two[:, rows - reach :], ahead)
    far_lo = hop(two[:, : rows - reach], odd_ahead)
    cross_hi = hop(far_hi, down)
    cross_lo = hop(far_lo, down)
    one = jnp.where(is_even, swapped, pair)
    three_hi = jnp.where(is_even, cross_hi, swapped[:, rows - reach :])
    three_lo = jnp.where(is_even, cross_lo, swapped[:, : rows - reach])
    return [far_hi, three_lo, three_hi, two, one, stacked]


def body(doc_lengths, queries, key_states, value_states):
    seq_rank = lax.axis_index("seq")
    rows = queries.shape[0]
    tiles = rows // TILE
    kv_heads = key_states.shape[1] // HD
    group = queries.shape[1] // (kv_heads * HD)
    width = group * TILE
    every_length = doubling_gather(doubling_gather(doc_lengths, "head"), "seq")
    positions = seq_rank * rows + jnp.arange(rows, dtype=jnp.int32)
    stacked = jnp.stack([key_states, value_states], axis=0)
    every_length, stacked = lax.optimization_barrier((every_length, stacked))
    doc_ends = jnp.cumsum(every_length)
    pieces = gather_window(stacked, lax.axis_size("seq"))
    starts = document_start(positions, doc_ends, every_length)
    piece_rows = [piece.shape[1] for piece in pieces]
    local_row = sum(piece_rows[:-1])
    start_rows = (starts - seq_rank * rows + local_row + PAD).reshape(tiles, TILE)
    tile_rows = PAD + local_row + jnp.arange(tiles, dtype=jnp.int32) * TILE
    total = jnp.maximum(0, tile_rows - start_rows[:, 0] + KB - 1) // KB
    plain = jnp.maximum(0, tile_rows - start_rows[:, -1]) // KB
    starts_wide = jnp.tile(start_rows, (1, CHUNK // TILE))

    win_rows = PAD + sum(piece_rows)
    kernel = functools.partial(attend, len(pieces), piece_rows, local_row, group)
    return pl.pallas_call(
        kernel,
        out_shape=jax.ShapeDtypeStruct(queries.shape, jnp.bfloat16),
        grid_spec=pltpu.PrefetchScalarGridSpec(
            num_scalar_prefetch=2,
            grid=(kv_heads, tiles),
            in_specs=[
                pl.BlockSpec((tiles, CHUNK), lambda c, t, *_: (0, 0)),
                pl.BlockSpec((TILE, width), lambda c, t, *_: (t, c)),
            ]
            + [pl.BlockSpec(memory_space=pl.ANY)] * len(pieces),
            out_specs=pl.BlockSpec((TILE, width), lambda c, t, *_: (t, c)),
            scratch_shapes=[
                pltpu.VMEM((2, kv_heads, win_rows, HD), jnp.bfloat16),
                pltpu.VMEM((width, HD), jnp.bfloat16),
                pltpu.VMEM((HD, width), jnp.float32),
                pltpu.VMEM((1, width), jnp.float32),
                pltpu.VMEM((1, width), jnp.float32),
                pltpu.SemaphoreType.DMA((len(pieces), 2, kv_heads)),
            ],
        ),
        compiler_params=pltpu.CompilerParams(
            dimension_semantics=("arbitrary", "arbitrary"), vmem_limit_bytes=48 * 1024 * 1024
        ),
    )(plain, total, starts_wide, queries, *pieces)


def solution(mesh):
    return jax.shard_map(
        body,
        mesh=mesh,
        in_specs=(P(("seq", "head")), P("seq", "head"), P("seq", "head"), P("seq", "head")),
        out_specs=P("seq", "head"),
        check_vma=False,
    )
```
